256 devices in a mesh: section: 2 (over y_hi), pen: 64 (over y_lo, z, x), slab: 2 (over core).
Axes of the slice: x: 4, y: 4 (y_hi: 2, y_lo: 2; y = y_hi * 2 + y_lo), z: 8, core: 2. Of those that a mesh axis runs over, the one named last changes fastest.
Arguments:
- velocity: float32 [3, 384, 384, 384], P(None, ('section', 'pen'), 'slab'), may hold values from -6 to 6
- vorticity: float32 [3, 384, 384, 384], P(None, ('section', 'pen'), 'slab'), may hold values from -6 to 6
- velocity_modes: float32 [3, 256, 256, 2, 256], P(None, None, ('section', 'pen'), None, 'slab'), may hold values from -6 to 6
Outputs:
- rhs_modes: float32 [3, 256, 256, 2, 256], P(None, None, ('section', 'pen'), None, 'slab')
The draws below stay inside these ranges and needn't reach their ends.
All inputs are finite; a program needn't handle non-finite values.
Results may differ from the reference program's by a relative error of at most 0.000057.
Values sent between devices are 32-bit elements; how exact they have to be, the bound alone decides.
A program may use at most 64 MiB of HBM per device.

```python
import jax
import jax.numpy as jnp
from jax import lax

N = 384
KEEP = 256


def block_levels(stream_key, shape, split, low, top_value):
    def one(position, blocks):
        steps = jax.random.uniform(jax.random.fold_in(jax.random.fold_in(stream_key, 6), position), (blocks,), jnp.float32, low / len(split), top_value / len(split))
        return jnp.repeat(jnp.exp(steps), shape[position] // blocks).reshape((-1,) + (1,) * (len(shape) - position - 1))

    loudness = one(*split[0])
    for cut in split[1:]:
        loudness = loudness * one(*cut)
    return loudness


def centred(stream_key, shape, deviation, most, split=(), kind=jnp.bfloat16):
    drawn = deviation * jax.random.normal(stream_key, shape, jnp.float32)
    if split:
        drawn = drawn * block_levels(stream_key, shape, split, -0.22, 0.18)
    return jnp.clip(drawn, -most, most).astype(kind)


def setup_inputs(seed: int = 0) -> dict:
    streams_of = jax.random.split(jax.random.key(seed), 4)
    return {
        "velocity": centred(streams_of[0], (3, N, N, N), 1.0, 6.0, ((1, 128), (2, 2)), jnp.float32),
        "vorticity": centred(streams_of[1], (3, N, N, N), 1.0, 6.0, ((1, 128), (2, 2)), jnp.float32),
        "velocity_modes": centred(streams_of[2], (3, KEEP, KEEP, 2, KEEP), 1.0, 6.0, ((2, 128), (4, 2)), jnp.float32),
    }


def signed_modes(index, count):
    return jnp.where(index < count // 2, index, index - count)


def reference(velocity, vorticity, velocity_modes):
    velocity_field = velocity
    vorticity_field = vorticity
    cross_product = jnp.stack([velocity_field[1] * vorticity_field[2] - velocity_field[2] * vorticity_field[1],
                         velocity_field[2] * vorticity_field[0] - velocity_field[0] * vorticity_field[2],
                         velocity_field[0] * vorticity_field[1] - velocity_field[1] * vorticity_field[0]])
    picked = jnp.concatenate([jnp.arange(KEEP // 2, dtype=jnp.int32),
                              jnp.arange(N - KEEP // 2, N, dtype=jnp.int32)])

    def transform(field):
        spec = jnp.fft.fft(field, axis=2, norm="ortho")[:, :, picked]
        spec = jnp.fft.fft(spec, axis=1, norm="ortho")[:, picked, :]
        spec = jnp.fft.fft(spec, axis=0, norm="ortho")[picked]
        return jnp.stack([jnp.real(spec), jnp.imag(spec)])

    spectrum = lax.map(transform, cross_product)
    modes = signed_modes(jnp.arange(KEEP, dtype=jnp.int32), KEEP)
    kz = modes[:, None, None]
    ky = modes[None, :, None]
    kx = modes[None, None, :]
    limit = -(KEEP // 2)
    mask = ((kx != limit) & (ky != limit) & (kz != limit)).astype(jnp.float32)
    waves = (kx.astype(jnp.float32), ky.astype(jnp.float32), kz.astype(jnp.float32))
    ksq = waves[0] * waves[0] + waves[1] * waves[1] + waves[2] * waves[2]
    denom = jnp.maximum(ksq, 1.0)
    parts = []
    for which in range(2):
        comp = [spectrum[c, which] for c in range(3)]
        inner = (waves[0] * comp[0] + waves[1] * comp[1] + waves[2] * comp[2]) / denom
        parts.append(jnp.stack([comp[c] - waves[c] * inner for c in range(3)]))
    projected = jnp.stack(parts, axis=3)
    visc = 0.5 / (KEEP // 2) ** 2
    return projected * mask[None, :, :, None, :] - visc * ksq[None, :, :, None, :] * velocity_modes
```

```python
import functools
import math

import jax
import jax.numpy as jnp
import numpy as np
from jax import lax
from jax.experimental import pallas as pl
from jax.experimental.pallas import tpu as pltpu
from jax.sharding import PartitionSpec as P

MESH = pl.DeviceIdType.MESH
f32, bf16 = jnp.float32, jnp.bfloat16


def signed(count):
    j = np.arange(count)
    return np.where(j < count // 2, j, j - count)


def high_low(table):
    high = table.astype(np.float32).astype(bf16)
    low = (table - high.astype(np.float64)).astype(np.float32).astype(bf16)
    return high, low


def tables(n, keep, devices):
    k = signed(keep)
    phase = 2.0 * math.pi / n * np.mod(k[:, None] * np.arange(n)[None, :], n)
    cos, sin = np.cos(phase) / math.sqrt(n), np.sin(phase) / math.sqrt(n)
    half = keep // 2
    tx = []
    for b in range(2):
        rows = slice(b * half, (b + 1) * half)
        high, low = high_low(np.concatenate([cos[rows].T, -sin[rows].T], axis=1))
        tx.append(np.concatenate([high, low, high], axis=0))
    ty = []
    for p in range(2):
        high, low = high_low(np.concatenate([cos[p::2, : n // 2], sin[p::2, : n // 2]], axis=0))
        ty.append(np.concatenate([high, low, high], axis=1))
    order = np.arange(n).reshape(devices, n // devices).T.reshape(-1)
    high, low = high_low(np.concatenate([cos[:, order], sin[:, order]], axis=0))
    tz = np.concatenate([high, low, high], axis=1)
    return np.stack(tx), np.stack(ty), tz


def split(x):
    high = x.astype(bf16)
    return high, (x - high.astype(f32)).astype(bf16)


def kernel(
    dims, v_hbm, w_hbm, m_hbm, tx_hbm, ty_hbm, tz_hbm, out,
    v, w, modes, tx, ty, tz, own, away, arrived, outbox, inbox, spec,
    in_sem, m_sem, t_sem, xs_sem, xr_sem, self_sem, s_sem, r_sem,
):
    ny, nz, nx, planes, keep, n = dims
    half = keep // 2
    group = ny * nz * nx
    quad = 4 * planes
    me = lax.axis_index("section") * (group // 2) + lax.axis_index("pen")
    slab = lax.axis_index("slab")
    mx, mz, my = me % nx, (me // nx) % nz, me // (nx * nz)

    def peer(i):
        j = i // (nx * ny)
        rest = i % (nx * ny)
        dz = nz // 2 + ((j + 1) // 2) * (2 * (j % 2) - 1)
        dy = ny // 2 + rest // nx
        dx = nx // 2 + rest % nx
        return ((my + dy) % ny) * (nx * nz) + ((mz + dz) % nz) * nx + (mx + dx) % nx

    def device(t, s):
        return {"section": t // (group // 2), "pen": t % (group // 2), "slab": s}

    self_step = (nz - 1) * nx * ny + (ny // 2) * nx + nx // 2

    def each_peer(body):
        def step(i, carry):
            body(peer(i + jnp.where(i >= self_step, 1, 0)))
            return carry

        lax.fori_loop(0, group - 1, step, 0)

    barrier = pltpu.get_barrier_semaphore()
    each_peer(
        lambda t: pl.semaphore_signal(barrier, inc=1, device_id=device(t, slab), device_id_type=MESH)
    )
    pl.semaphore_signal(barrier, inc=1, device_id=device(me, 1 - slab), device_id_type=MESH)

    loads = [
        pltpu.make_async_copy(tx_hbm, tx, t_sem.at[0]),
        pltpu.make_async_copy(ty_hbm, ty, t_sem.at[1]),
        pltpu.make_async_copy(tz_hbm, tz, t_sem.at[2]),
    ]
    loads[0].start()
    inputs = {}
    for c in (1, 2, 0):
        for i, (src, dst) in enumerate(((v_hbm, v), (w_hbm, w))):
            inputs[c, i] = pltpu.make_async_copy(src.at[c], dst.at[c], in_sem.at[2 * c + i])
            inputs[c, i].start()
    loads[1].start()
    loads[2].start()
    mode_load = pltpu.make_async_copy(m_hbm, modes, m_sem)
    mode_load.start()

    loads[0].wait()
    for c in range(3):
        a, b = (c + 1) % 3, (c + 2) % 3
        if c == 0:
            for key in ((1, 0), (1, 1), (2, 0), (2, 1)):
                inputs[key].wait()
        if c == 1:
            for key in ((0, 0), (0, 1)):
                inputs[key].wait()

        def x_plane(z, carry, a=a, b=b, c=c):
            p = v[a, z] * w[b, z] - v[b, z] * w[a, z]
            high, low = split(p)
            lhs = jnp.concatenate([high, high, low], axis=1)
            away[c * planes + z] = jnp.dot(lhs, tx[1 - slab], preferred_element_type=f32)
            own[c * planes + z] = jnp.dot(lhs, tx[slab], preferred_element_type=f32)
            return carry

        lax.fori_loop(0, planes, x_plane, 0)

    pl.semaphore_wait(barrier, group)

    def swap(p):
        return pltpu.make_async_remote_copy(
            src_ref=away.at[p],
            dst_ref=arrived.at[p],
            send_sem=xs_sem.at[p],
            recv_sem=xr_sem.at[p],
            device_id=device(me, 1 - slab),
            device_id_type=MESH,
        )

    for p in range(3 * planes):
        swap(p).start()
    loads[1].wait()
    sign = (1 - 2 * slab).astype(f32)

    def component(c, carry):
        def y_plane(z, carry):
            p = c * planes + z
            swap(p).wait_recv()
            mine, other = own[p], arrived[p]
            for parity, folded in enumerate((mine + other, sign * (mine - other))):
                high, low = split(folded)
                both = jnp.dot(
                    ty[parity],
                    jnp.concatenate([high, high, low], axis=0),
                    preferred_element_type=f32,
                )
                row = z * 4 + parity * 2
                outbox[c, pl.ds(row, half, stride=quad), :] = both[:half, :half] + both[half:, half:]
                outbox[c, pl.ds(row + 1, half, stride=quad), :] = (
                    both[:half, half:] - both[half:, :half]
                )
            return carry

        lax.fori_loop(0, planes, y_plane, 0)

        def send(t):
            pltpu.make_async_remote_copy(
                src_ref=outbox.at[c, pl.ds(t * quad, quad)],
                dst_ref=inbox.at[c, pl.ds(me * quad, quad)],
                send_sem=s_sem.at[c],
                recv_sem=r_sem.at[c],
                device_id=device(t, slab),
                device_id_type=MESH,
            ).start()

        each_peer(send)
        pltpu.make_async_copy(
            outbox.at[c, pl.ds(me * quad, quad)], inbox.at[c, pl.ds(me * quad, quad)], self_sem.at[c]
        ).start()
        return carry

    lax.fori_loop(0, 3, component, 0)
    loads[2].wait()

    def z_component(c, carry):
        some = pl.ds(0, (group - 1) * quad)
        pltpu.make_async_copy(outbox.at[c, some], inbox.at[c, some], r_sem.at[c]).wait()
        pltpu.make_async_copy(
            outbox.at[c, pl.ds(me * quad, quad)], inbox.at[c, pl.ds(me * quad, quad)], self_sem.at[c]
        ).wait()
        for q in range(2):
            pieces = [
                jnp.concatenate(
                    [inbox[c, pl.ds(r * 4 + q * 2 + part, group, stride=quad), :] for r in range(planes)],
                    axis=0,
                )
                for part in range(2)
            ]
            high, low = split(jnp.concatenate(pieces, axis=1))
            both = jnp.dot(
                tz[...], jnp.concatenate([high, high, low], axis=0), preferred_element_type=f32
            )
            spec[c, 2 * q] = both[:keep, :half] + both[keep:, half:]
            spec[c, 2 * q + 1] = both[:keep, half:] - both[keep:, :half]
        return carry

    lax.fori_loop(0, 3, z_component, 0)
    mode_load.wait()

    limit = -half
    to_wave = lambda j: jnp.where(j < half, j, j - keep)
    kz = to_wave(lax.broadcasted_iota(jnp.int32, (keep, half), 0))
    kx = to_wave(slab * half + lax.broadcasted_iota(jnp.int32, (keep, half), 1))
    visc = 0.5 / half**2
    for q in range(2):
        ky = jnp.full((keep, half), to_wave(2 * me + q), jnp.int32)
        kept = ((kx != limit) & (ky != limit) & (kz != limit)).astype(f32)
        waves = (kx.astype(f32), ky.astype(f32), kz.astype(f32))
        ksq = waves[0] * waves[0] + waves[1] * waves[1] + waves[2] * waves[2]
        scale = 1.0 / jnp.maximum(ksq, 1.0)
        for part in range(2):
            row = 2 * q + part
            s = [spec[c, row] for c in range(3)]
            inner = (waves[0] * s[0] + waves[1] * s[1] + waves[2] * s[2]) * scale
            for c in range(3):
                rows = pl.ds(row, keep, stride=4)
                out[c, rows, :] = (s[c] - waves[c] * inner) * kept - visc * ksq * modes[c, rows, :]

    for p in range(3 * planes):
        swap(p).wait_send()
    for c in range(3):
        some = pl.ds(0, (group - 1) * quad)
        pltpu.make_async_copy(outbox.at[c, some], inbox.at[c, some], s_sem.at[c]).wait()


def per_device(sizes, velocity, vorticity, velocity_modes):
    ny, nz, nx = sizes
    _, planes, rows, n = velocity.shape
    keep, half = velocity_modes.shape[1], velocity_modes.shape[4]
    group = ny * nz * nx
    tx, ty, tz = tables(n, keep, group)
    anywhere = pl.BlockSpec(memory_space=pl.ANY)
    quad = 4 * planes
    dma = pltpu.SemaphoreType.DMA
    out = pl.pallas_call(
        functools.partial(kernel, (ny, nz, nx, planes, keep, n)),
        out_shape=jax.ShapeDtypeStruct((3, 4 * keep, half), f32),
        in_specs=[anywhere] * 6,
        out_specs=pl.BlockSpec(memory_space=pltpu.VMEM),
        scratch_shapes=[
            pltpu.VMEM((3, planes, rows, n), f32),
            pltpu.VMEM((3, planes, rows, n), f32),
            pltpu.VMEM((3, 4 * keep, half), f32),
            pltpu.VMEM(tx.shape, bf16),
            pltpu.VMEM(ty.shape, bf16),
            pltpu.VMEM(tz.shape, bf16),
            pltpu.VMEM((3 * planes, rows, keep), f32),
            pltpu.VMEM((3 * planes, rows, keep), f32),
            pltpu.VMEM((3 * planes, rows, keep), f32),
            pltpu.VMEM((3, group * quad, half), f32),
            pltpu.VMEM((3, group * quad, half), f32),
            pltpu.VMEM((3, 4, keep, half), f32),
            dma((6,)),
            dma,
            dma((3,)),
            dma((3 * planes,)),
            dma((3 * planes,)),
            dma((3,)),
            dma((3,)),
            dma((3,)),
        ],
        compiler_params=pltpu.CompilerParams(
            collective_id=0, has_side_effects=True, vmem_limit_bytes=60 << 20
        ),
    )(velocity, vorticity, velocity_modes.reshape(3, 4 * keep, half), tx, ty, tz)
    return out.reshape(velocity_modes.shape)


def solution(mesh):
    sizes = (4, 8, 4)
    return jax.shard_map(
        functools.partial(per_device, sizes),
        mesh=mesh,
        in_specs=(
            P(None, ("section", "pen"), "slab", None),
            P(None, ("section", "pen"), "slab", None),
            P(None, None, ("section", "pen"), None, "slab"),
        ),
        out_specs=P(None, None, ("section", "pen"), None, "slab"),
        check_vma=False,
    )
```

```python
import functools
import math

import jax
import jax.numpy as jnp
import numpy as np
from jax import lax
from jax.experimental import pallas as pl
from jax.experimental.pallas import tpu as pltpu
from jax.sharding import PartitionSpec as P

MESH = pl.DeviceIdType.MESH
f32, bf16 = jnp.float32, jnp.bfloat16


def signed(count):
    j = np.arange(count)
    return np.where(j < count // 2, j, j - count)


def high_low(table):
    high = table.astype(np.float32).astype(bf16)
    low = (table - high.astype(np.float64)).astype(np.float32).astype(bf16)
    return high, low


def tables(n, keep, devices):
    k = signed(keep)
    phase = 2.0 * math.pi / n * np.mod(k[:, None] * np.arange(n)[None, :], n)
    cos, sin = np.cos(phase) / math.sqrt(n), np.sin(phase) / math.sqrt(n)
    half = keep // 2
    tx = []
    for b in range(2):
        rows = slice(b * half, (b + 1) * half)
        high, low = high_low(np.concatenate([cos[rows].T, -sin[rows].T], axis=1))
        tx.append(np.concatenate([high, low, high], axis=0))
    ty = []
    for p in range(2):
        high, low = high_low(np.concatenate([cos[p::2, : n // 2], sin[p::2, : n // 2]], axis=0))
        ty.append(np.concatenate([high, low, high], axis=1))
    order = np.arange(n).reshape(devices, n // devices).T.reshape(-1)
    high, low = high_low(np.concatenate([cos[:, order], sin[:, order]], axis=0))
    tz = np.concatenate([high, low, high], axis=1)
    return np.stack(tx), np.stack(ty), tz


def split(x):
    high = x.astype(bf16)
    return high, (x - high.astype(f32)).astype(bf16)


def kernel(
    dims, v_hbm, w_hbm, tx_hbm, ty_hbm, tz_hbm, out,
    v, w, tx, ty, tz, own, away, arrived, outbox, inbox, spec,
    in_sem, t_sem, xs_sem, xr_sem, self_sem, s_sem, r_sem, plane_sem, all_sem,
):
    ny, nz, nx, planes, keep, n = dims
    half = keep // 2
    group = ny * nz * nx
    quad = 4 * planes
    me = lax.axis_index("section") * (group // 2) + lax.axis_index("pen")
    slab = lax.axis_index("slab")
    mx, mz, my = me & (nx - 1), (me // nx) & (nz - 1), me // (nx * nz)

    def device(t, s):
        return {"section": t // (group // 2), "pen": t & (group // 2 - 1), "slab": s}

    far_first = [nz // 2 + ((j + 1) // 2) * (2 * (j % 2) - 1) for j in range(nz)]

    def each_peer(body, steps=far_first):
        for dz in steps:
            line = ((mz + dz) & (nz - 1)) * nx

            def step(i, carry, line=line):
                ty = (my + i // nx) & (ny - 1)
                tx = (mx + i) & (nx - 1)
                body(ty * (nx * nz) + line + tx)
                return carry

            lax.fori_loop(1 if dz % nz == 0 else 0, nx * ny, step, 0)

    loads = [
        pltpu.make_async_copy(tx_hbm, tx, t_sem.at[0]),
        pltpu.make_async_copy(ty_hbm, ty, t_sem.at[1]),
        pltpu.make_async_copy(tz_hbm, tz, t_sem.at[2]),
    ]
    inputs = {}
    for c in (1, 2, 0):
        for i, (src, dst) in enumerate(((v_hbm, v), (w_hbm, w))):
            inputs[c, i] = pltpu.make_async_copy(src.at[c], dst.at[c], in_sem.at[2 * c + i])
            inputs[c, i].start()
        if c == 2:
            loads[0].start()
    loads[1].start()
    loads[2].start()

    barrier = pltpu.get_barrier_semaphore()

    def greet(t, semaphore, s=slab):
        pl.semaphore_signal(semaphore, inc=1, device_id=device(t, s), device_id_type=MESH)

    def across_z():
        return [my * (nx * nz) + ((mz + d) & (nz - 1)) * nx + mx for d in far_first if d % nz]

    def across_x():
        return [me - mx + ((mx + d) & (nx - 1)) for d in (2, 1, 3)]

    def across_y():
        return [((my + d) & (ny - 1)) * (nx * nz) + mz * nx + mx for d in (2, 1, 3)]

    with jax.named_scope("greet"):
        lines = across_z() + across_x() + across_y()
        for t in lines:
            greet(t, barrier)
        greet(me, barrier, 1 - slab)

    def swap(p):
        return pltpu.make_async_remote_copy(
            src_ref=away.at[p],
            dst_ref=arrived.at[p],
            send_sem=xs_sem.at[p],
            recv_sem=xr_sem.at[p],
            device_id=device(me, 1 - slab),
            device_id_type=MESH,
        )

    def x_component(c):
        a, b = (c + 1) % 3, (c + 2) % 3

        def x_plane(z, carry):
            p = v[a, z] * w[b, z] - v[b, z] * w[a, z]
            high, low = split(p)
            lhs = jnp.concatenate([high, high, low], axis=1)
            away[c * planes + z] = jnp.dot(lhs, tx[1 - slab], preferred_element_type=f32)
            own[c * planes + z] = jnp.dot(lhs, tx[slab], preferred_element_type=f32)
            return carry

        with jax.named_scope("x"):
            lax.fori_loop(0, planes, x_plane, 0)

    sign = (1 - 2 * slab).astype(f32)

    def y_component(c):
        def y_plane(z, carry):
            p = c * planes + z
            swap(p).wait_recv()
            mine, other = own[p], arrived[p]
            for parity, folded in enumerate((mine + other, sign * (mine - other))):
                high, low = split(folded)
                both = jnp.dot(
                    ty[parity],
                    jnp.concatenate([high, high, low], axis=0),
                    preferred_element_type=f32,
                )
                row = z * 4 + parity * 2
                outbox[c, pl.ds(row, half, stride=quad), :] = both[:half, :half] + both[half:, half:]
                outbox[c, pl.ds(row + 1, half, stride=quad), :] = (
                    both[:half, half:] - both[half:, :half]
                )
            return carry

        with jax.named_scope("y"):
            lax.fori_loop(0, planes, y_plane, 0)

    def send_component(c):
        def send(t):
            pltpu.make_async_remote_copy(
                src_ref=outbox.at[c, pl.ds(t * quad, quad)],
                dst_ref=inbox.at[c, pl.ds(me * quad, quad)],
                send_sem=s_sem.at[c],
                recv_sem=r_sem.at[c],
                device_id=device(t, slab),
                device_id_type=MESH,
            ).start()

        with jax.named_scope("send"):
            each_peer(send)
        pltpu.make_async_copy(
            outbox.at[c, pl.ds(me * quad, quad)], inbox.at[c, pl.ds(me * quad, quad)], self_sem.at[c]
        ).start()

    def swap_component(c):
        for z in range(planes):
            swap(c * planes + z).start()

    for key in ((1, 0), (1, 1), (2, 0), (2, 1)):
        inputs[key].wait()
    loads[0].wait()
    x_component(0)
    with jax.named_scope("lines"):
        pl.semaphore_wait(barrier, len(lines) + 1)
    swap_component(0)
    for t in across_x():
        greet(t, plane_sem)
    for key in ((0, 0), (0, 1)):
        inputs[key].wait()
    x_component(1)
    swap_component(1)
    with jax.named_scope("plane"):
        pl.semaphore_wait(plane_sem, nx - 1)
    for t in across_y():
        greet(t, all_sem)
    loads[1].wait()
    y_component(0)
    with jax.named_scope("all"):
        pl.semaphore_wait(all_sem, ny - 1)
    send_component(0)
    x_component(2)
    swap_component(2)
    y_component(1)
    send_component(1)
    y_component(2)
    send_component(2)
    loads[2].wait()

    def z_component(c, carry):
        some = pl.ds(0, (group - 1) * quad)
        with jax.named_scope("recv"):
            pltpu.make_async_copy(outbox.at[c, some], inbox.at[c, some], r_sem.at[c]).wait()
        pltpu.make_async_copy(
            outbox.at[c, pl.ds(me * quad, quad)], inbox.at[c, pl.ds(me * quad, quad)], self_sem.at[c]
        ).wait()
        with jax.named_scope("z"):
            for q in range(2):
                pieces = [
                    jnp.concatenate(
                        [inbox[c, pl.ds(r * 4 + q * 2 + part, group, stride=quad), :] for r in range(planes)],
                        axis=0,
                    )
                    for part in range(2)
                ]
                high, low = split(jnp.concatenate(pieces, axis=1))
                both = jnp.dot(
                    tz[...], jnp.concatenate([high, high, low], axis=0), preferred_element_type=f32
                )
                spec[c, 2 * q] = both[:keep, :half] + both[keep:, half:]
                spec[c, 2 * q + 1] = both[:keep, half:] - both[keep:, :half]
        return carry

    lax.fori_loop(0, 3, z_component, 0)

    limit = -half
    to_wave = lambda j: jnp.where(j < half, j, j - keep)
    kz = to_wave(lax.broadcasted_iota(jnp.int32, (keep, half), 0))
    kx = to_wave(slab * half + lax.broadcasted_iota(jnp.int32, (keep, half), 1))
    with jax.named_scope("project"):
        for q in range(2):
            ky = jnp.full((keep, half), to_wave(2 * me + q), jnp.int32)
            kept = ((kx != limit) & (ky != limit) & (kz != limit)).astype(f32)
            waves = (kx.astype(f32), ky.astype(f32), kz.astype(f32))
            ksq = waves[0] * waves[0] + waves[1] * waves[1] + waves[2] * waves[2]
            scale = 1.0 / jnp.maximum(ksq, 1.0)
            for part in range(2):
                row = 2 * q + part
                s = [spec[c, row] for c in range(3)]
                inner = (waves[0] * s[0] + waves[1] * s[1] + waves[2] * s[2]) * scale
                for c in range(3):
                    rows = pl.ds(row, keep, stride=4)
                    out[c, rows, :] = (s[c] - waves[c] * inner) * kept
    with jax.named_scope("drain"):
        for p in range(3 * planes):
            swap(p).wait_send()
        for c in range(3):
            some = pl.ds(0, (group - 1) * quad)
            pltpu.make_async_copy(outbox.at[c, some], inbox.at[c, some], s_sem.at[c]).wait()


def per_device(sizes, velocity, vorticity, velocity_modes):
    ny, nz, nx = sizes
    _, planes, rows, n = velocity.shape
    keep, half = velocity_modes.shape[1], velocity_modes.shape[4]
    group = ny * nz * nx
    tx, ty, tz = tables(n, keep, group)
    anywhere = pl.BlockSpec(memory_space=pltpu.HBM)
    quad = 4 * planes
    dma = pltpu.SemaphoreType.DMA
    out = pl.pallas_call(
        functools.partial(kernel, (ny, nz, nx, planes, keep, n)),
        out_shape=jax.ShapeDtypeStruct((3, 4 * keep, half), f32),
        in_specs=[anywhere] * 5,
        out_specs=pl.BlockSpec(memory_space=pltpu.VMEM),
        scratch_shapes=[
            pltpu.VMEM((3, planes, rows, n), f32),
            pltpu.VMEM((3, planes, rows, n), f32),
            pltpu.VMEM(tx.shape, bf16),
            pltpu.VMEM(ty.shape, bf16),
            pltpu.VMEM(tz.shape, bf16),
            pltpu.VMEM((3 * planes, rows, keep), f32),
            pltpu.VMEM((3 * planes, rows, keep), f32),
            pltpu.VMEM((3 * planes, rows, keep), f32),
            pltpu.VMEM((3, group * quad, half), f32),
            pltpu.VMEM((3, group * quad, half), f32),
            pltpu.VMEM((3, 4, keep, half), f32),
            dma((6,)),
            dma((3,)),
            dma((3 * planes,)),
            dma((3 * planes,)),
            dma((3,)),
            dma((3,)),
            dma((3,)),
            pltpu.SemaphoreType.REGULAR,
            pltpu.SemaphoreType.REGULAR,
        ],
        compiler_params=pltpu.CompilerParams(
            collective_id=0, has_side_effects=True, vmem_limit_bytes=28 << 20
        ),
    )(*(pltpu.with_memory_space_constraint(x, pltpu.HBM) for x in (velocity, vorticity, tx, ty, tz)))
    shape = (4 * keep, half)
    row = lax.broadcasted_iota(jnp.int32, shape, 0)
    me = lax.axis_index("section") * (group // 2) + lax.axis_index("pen")
    to_wave = lambda j: jnp.where(j < half, j, j - keep).astype(f32)
    kz, ky = to_wave(row // 4), to_wave(2 * me + (row // 2) % 2)
    kx = to_wave(lax.axis_index("slab") * half + lax.broadcasted_iota(jnp.int32, shape, 1))
    viscous = 0.5 / half**2 * (kx * kx + ky * ky + kz * kz)
    rhs = out - viscous * velocity_modes.reshape(3, *shape)
    return rhs.reshape(velocity_modes.shape)


def solution(mesh):
    sizes = (4, 8, 4)
    return jax.shard_map(
        functools.partial(per_device, sizes),
        mesh=mesh,
        in_specs=(
            P(None, ("section", "pen"), "slab", None),
            P(None, ("section", "pen"), "slab", None),
            P(None, None, ("section", "pen"), None, "slab"),
        ),
        out_specs=P(None, None, ("section", "pen"), None, "slab"),
        check_vma=False,
    )
```

```python
import functools
import math

import jax
import jax.numpy as jnp
import numpy as np
from jax import lax
from jax.experimental import pallas as pl
from jax.experimental.pallas import tpu as pltpu
from jax.sharding import PartitionSpec as P

MESH = pl.DeviceIdType.MESH
f32, bf16 = jnp.float32, jnp.bfloat16


def signed(count):
    j = np.arange(count)
    return np.where(j < count // 2, j, j - count)


def high_low(table):
    high = table.astype(np.float32).astype(bf16)
    low = (table - high.astype(np.float64)).astype(np.float32).astype(bf16)
    return high, low


def tables(n, keep, devices):
    k = signed(keep)
    phase = 2.0 * math.pi / n * np.mod(k[:, None] * np.arange(n)[None, :], n)
    cos, sin = np.cos(phase) / math.sqrt(n), np.sin(phase) / math.sqrt(n)
    half = keep // 2
    tx = []
    for b in range(2):
        rows = slice(b * half, (b + 1) * half)
        high, low = high_low(np.concatenate([cos[rows].T, -sin[rows].T], axis=1))
        tx.append(np.concatenate([high, low, high], axis=0))
    ty = []
    for p in range(2):
        high, low = high_low(np.concatenate([cos[p::2, : n // 2], sin[p::2, : n // 2]], axis=0))
        ty.append(np.concatenate([high, low, high], axis=1))
    order = np.arange(n).reshape(devices, n // devices).T.reshape(-1)
    high, low = high_low(np.concatenate([cos[:, order], sin[:, order]], axis=0))
    tz = np.concatenate([high, low, high], axis=1)
    return np.stack(tx), np.stack(ty), tz


def split(x):
    high = x.astype(bf16)
    return high, (x - high.astype(f32)).astype(bf16)


def kernel(
    dims, v_hbm, w_hbm, m_hbm, tx_hbm, ty_hbm, tz_hbm, out, viscous,
    v, w, modes, tx, ty, tz, own, away, arrived, outbox, inbox, spec,
    in_sem, m_sem, t_sem, xs_sem, xr_sem, self_sem, s_sem, r_sem, plane_sem, all_sem,
):
    ny, nz, nx, planes, keep, n = dims
    half = keep // 2
    group = ny * nz * nx
    quad = 4 * planes
    me = lax.axis_index("section") * (group // 2) + lax.axis_index("pen")
    slab = lax.axis_index("slab")
    mx, mz, my = me & (nx - 1), (me // nx) & (nz - 1), me // (nx * nz)

    def device(t, s):
        return {"section": t // (group // 2), "pen": t & (group // 2 - 1), "slab": s}

    far_first = [nz // 2 + ((j + 1) // 2) * (2 * (j % 2) - 1) for j in range(nz)]

    def far(j, count):
        return count // 2 + ((j + 1) // 2) * (2 * (j & 1) - 1)

    def each_peer(body, first=0, last=nx * ny):
        def step(i, carry):
            ty = (my + far(i // nx, ny)) & (ny - 1)
            tx = (mx + far(i & (nx - 1), nx)) & (nx - 1)
            for dz in far_first:
                body(ty * (nx * nz) + ((mz + dz) & (nz - 1)) * nx + tx)
            return carry

        lax.fori_loop(first, min(last, nx * ny - 1), step, 0)
        if last == nx * ny:
            for dz in far_first:
                if dz % nz:
                    body(me - mz * nx + ((mz + dz) & (nz - 1)) * nx)

    x_table = pltpu.make_async_copy(tx_hbm, tx, t_sem.at[0])
    y_table = pltpu.make_async_copy(ty_hbm, ty, t_sem.at[1])
    z_table = pltpu.make_async_copy(tz_hbm, tz, t_sem.at[2])
    mode_load = pltpu.make_async_copy(m_hbm, modes, m_sem)
    fields = [
        [
            pltpu.make_async_copy(src.at[c, z], dst.at[c, z], in_sem.at[4 * z + i])
            for i, (src, dst, c) in enumerate(
                ((v_hbm, v, 1), (w_hbm, w, 2), (v_hbm, v, 2), (w_hbm, w, 1))
            )
        ]
        for z in range(planes)
    ] + [
        [
            pltpu.make_async_copy(src.at[0], dst.at[0], in_sem.at[4 * planes + i])
            for i, (src, dst) in enumerate(((v_hbm, v), (w_hbm, w)))
        ]
    ]

    def start(*copies):
        for copy in copies:
            copy.start()

    start(*fields[0], x_table)

    barrier = pltpu.get_barrier_semaphore()

    def greet(t, semaphore, s=slab):
        pl.semaphore_signal(semaphore, inc=1, device_id=device(t, s), device_id_type=MESH)

    def across_z():
        return [my * (nx * nz) + ((mz + d) & (nz - 1)) * nx + mx for d in far_first if d % nz]

    def across_x():
        return [me - mx + ((mx + d) & (nx - 1)) for d in (2, 1, 3)]

    def across_y():
        return [((my + d) & (ny - 1)) * (nx * nz) + mz * nx + mx for d in (2, 1, 3)]

    with jax.named_scope("greet"):
        lines = across_z() + across_x() + across_y()
        for t in lines:
            greet(t, barrier)
        greet(me, barrier, 1 - slab)
    start(*fields[1])

    def swap(p):
        return pltpu.make_async_remote_copy(
            src_ref=away.at[p],
            dst_ref=arrived.at[p],
            send_sem=xs_sem.at[p],
            recv_sem=xr_sem.at[p],
            device_id=device(me, 1 - slab),
            device_id_type=MESH,
        )

    def x_plane(c, z):
        a, b = (c + 1) % 3, (c + 2) % 3
        p = v[a, z] * w[b, z] - v[b, z] * w[a, z]
        high, low = split(p)
        lhs = jnp.concatenate([high, high, low], axis=1)
        away[c * planes + z] = jnp.dot(lhs, tx[1 - slab], preferred_element_type=f32)
        own[c * planes + z] = jnp.dot(lhs, tx[slab], preferred_element_type=f32)

    sign = (1 - 2 * slab).astype(f32)

    def row_of(c, z, q, part):
        return q * 2 * planes + z * 2 + part if c == 2 else z * 4 + q * 2 + part

    def y_plane(c, z):
        p = c * planes + z
        swap(p).wait_recv()
        mine, other = own[p], arrived[p]
        for q, folded in enumerate((mine + other, sign * (mine - other))):
            high, low = split(folded)
            both = jnp.dot(
                ty[q],
                jnp.concatenate([high, high, low], axis=0),
                preferred_element_type=f32,
            )
            outbox[c, pl.ds(row_of(c, z, q, 0), half, stride=quad), :] = (
                both[:half, :half] + both[half:, half:]
            )
            outbox[c, pl.ds(row_of(c, z, q, 1), half, stride=quad), :] = (
                both[:half, half:] - both[half:, :half]
            )

    def send(c, part, row, rows, **which):
        def one(t):
            pltpu.make_async_remote_copy(
                src_ref=outbox.at[c, pl.ds(t * quad + row, rows)],
                dst_ref=inbox.at[c, pl.ds(me * quad + row, rows)],
                send_sem=s_sem.at[part],
                recv_sem=r_sem.at[part],
                device_id=device(t, slab),
                device_id_type=MESH,
            ).start()

        with jax.named_scope("send"):
            each_peer(one, **which)

    def keep_own(c):
        return pltpu.make_async_copy(
            outbox.at[c, pl.ds(me * quad, quad)], inbox.at[c, pl.ds(me * quad, quad)], self_sem.at[c]
        )

    def looped(body, c):
        def step(z, carry):
            body(c, z)
            return carry

        lax.fori_loop(0, planes, step, 0)

    with jax.named_scope("x0"):
        for z in range(planes):
            for copy in fields[z]:
                copy.wait()
            if z == 0:
                x_table.wait()
                start(*fields[2], y_table, *fields[3])
            x_plane(0, z)
            if z == 0:
                with jax.named_scope("lines"):
                    pl.semaphore_wait(barrier, len(lines) + 1)
                for t in across_x():
                    greet(t, plane_sem)
            swap(z).start()
    start(z_table, mode_load)
    for copy in fields[planes]:
        copy.wait()
    x_plane(1, 0)
    with jax.named_scope("plane"):
        pl.semaphore_wait(plane_sem, nx - 1)
    for t in across_y():
        greet(t, all_sem)
    y_table.wait()
    for z in range(planes):
        with jax.named_scope("y0"):
            y_plane(0, z)
        send(0, 0, z * 4, 4, first=nx * (ny - 1))
    with jax.named_scope("all"):
        pl.semaphore_wait(all_sem, ny - 1)
    send(0, 0, 0, quad, last=nx * (ny - 1))
    keep_own(0).start()
    swap(planes).start()
    for z in range(1, planes):
        x_plane(1, z)
        swap(planes + z).start()
    with jax.named_scope("y1"):
        looped(y_plane, 1)
    send(1, 1, 0, quad)
    keep_own(1).start()
    with jax.named_scope("x2"):
        looped(x_plane, 2)
    for z in range(planes):
        swap(2 * planes + z).start()
    with jax.named_scope("y2"):
        looped(y_plane, 2)
    for q in range(2):
        send(2, 2 + q, q * 2 * planes, 2 * planes)
    keep_own(2).start()

    limit = -half
    visc = 0.5 / half**2
    to_wave = lambda j: jnp.where(j < half, j, j - keep)
    kz = to_wave(lax.broadcasted_iota(jnp.int32, (keep, half), 0))
    kx = to_wave(slab * half + lax.broadcasted_iota(jnp.int32, (keep, half), 1))

    def waves_of(q):
        ky = jnp.full((keep, half), to_wave(2 * me + q), jnp.int32)
        kept = ((kx != limit) & (ky != limit) & (kz != limit)).astype(f32)
        waves = (kx.astype(f32), ky.astype(f32), kz.astype(f32))
        ksq = waves[0] * waves[0] + waves[1] * waves[1] + waves[2] * waves[2]
        return waves, ksq, kept

    mode_load.wait()
    with jax.named_scope("viscous"):
        for q in range(2):
            _, ksq, _ = waves_of(q)
            for part in range(2):
                rows = pl.ds(2 * q + part, keep, stride=4)
                for c in range(3):
                    viscous[c, rows, :] = visc * ksq * modes[c, rows, :]
    z_table.wait()

    def z_rows(c, q):
        pieces = [
            jnp.concatenate(
                [inbox[c, pl.ds(row_of(c, r, q, part), group, stride=quad), :] for r in range(planes)],
                axis=0,
            )
            for part in range(2)
        ]
        high, low = split(jnp.concatenate(pieces, axis=1))
        parts = jnp.concatenate([high, high, low], axis=0)
        cos = jnp.dot(tz[:keep], parts, preferred_element_type=f32)
        sin = jnp.dot(tz[keep:], parts, preferred_element_type=f32)
        spec[c, 2 * q] = cos[:, :half] + sin[:, half:]
        spec[c, 2 * q + 1] = cos[:, half:] - sin[:, :half]

    def project(q):
        waves, ksq, kept = waves_of(q)
        scale = 1.0 / jnp.maximum(ksq, 1.0)
        for part in range(2):
            row = 2 * q + part
            s = [spec[c, row] for c in range(3)]
            inner = (waves[0] * s[0] + waves[1] * s[1] + waves[2] * s[2]) * scale
            for c in range(3):
                out[c, pl.ds(row, keep, stride=4), :] = (s[c] - waves[c] * inner) * kept

    def arrived_bytes(c, part, rows, sem):
        some = pl.ds(0, (group - 1) * rows)
        pltpu.make_async_copy(outbox.at[c, some], inbox.at[c, some], sem.at[part]).wait()

    for c in range(2):
        with jax.named_scope("recv"):
            arrived_bytes(c, c, quad, r_sem)
        keep_own(c).wait()
        with jax.named_scope("z"):
            for q in range(2):
                z_rows(c, q)
    keep_own(2).wait()
    for q in range(2):
        with jax.named_scope("recv"):
            arrived_bytes(2, 2 + q, 2 * planes, r_sem)
        with jax.named_scope("z"):
            z_rows(2, q)
        with jax.named_scope("project"):
            project(q)

    with jax.named_scope("drain"):
        for p in range(3 * planes):
            swap(p).wait_send()
        for part, (c, rows) in enumerate(((0, quad), (1, quad), (2, 2 * planes), (2, 2 * planes))):
            arrived_bytes(c, part, rows, s_sem)


def per_device(sizes, velocity, vorticity, velocity_modes):
    ny, nz, nx = sizes
    _, planes, rows, n = velocity.shape
    keep, half = velocity_modes.shape[1], velocity_modes.shape[4]
    group = ny * nz * nx
    tx, ty, tz = tables(n, keep, group)
    quad = 4 * planes
    dma = pltpu.SemaphoreType.DMA
    whole = jax.ShapeDtypeStruct((3, 4 * keep, half), f32)
    operands = (velocity, vorticity, velocity_modes.reshape(whole.shape), tx, ty, tz)
    projected, viscous = pl.pallas_call(
        functools.partial(kernel, (ny, nz, nx, planes, keep, n)),
        out_shape=(whole, whole),
        in_specs=[pl.BlockSpec(memory_space=pltpu.HBM)] * 6,
        out_specs=(pl.BlockSpec(memory_space=pltpu.VMEM),) * 2,
        scratch_shapes=[
            pltpu.VMEM((3, planes, rows, n), f32),
            pltpu.VMEM((3, planes, rows, n), f32),
            pltpu.VMEM(whole.shape, f32),
            pltpu.VMEM(tx.shape, bf16),
            pltpu.VMEM(ty.shape, bf16),
            pltpu.VMEM(tz.shape, bf16),
            pltpu.VMEM((3 * planes, rows, keep), f32),
            pltpu.VMEM((3 * planes, rows, keep), f32),
            pltpu.VMEM((3 * planes, rows, keep), f32),
            pltpu.VMEM((3, group * quad, half), f32),
            pltpu.VMEM((3, group * quad, half), f32),
            pltpu.VMEM((3, 4, keep, half), f32),
            dma((4 * planes + 2,)),
            dma,
            dma((3,)),
            dma((3 * planes,)),
            dma((3 * planes,)),
            dma((3,)),
            dma((4,)),
            dma((4,)),
            pltpu.SemaphoreType.REGULAR,
            pltpu.SemaphoreType.REGULAR,
        ],
        compiler_params=pltpu.CompilerParams(
            collective_id=0, has_side_effects=True, vmem_limit_bytes=30 << 20
        ),
    )(*(pltpu.with_memory_space_constraint(x, pltpu.HBM) for x in operands))
    return (projected - viscous).reshape(velocity_modes.shape)


def solution(mesh):
    sizes = (4, 8, 4)
    return jax.shard_map(
        functools.partial(per_device, sizes),
        mesh=mesh,
        in_specs=(
            P(None, ("section", "pen"), "slab", None),
            P(None, ("section", "pen"), "slab", None),
            P(None, None, ("section", "pen"), None, "slab"),
        ),
        out_specs=P(None, None, ("section", "pen"), None, "slab"),
        check_vma=False,
    )
```

```python
import functools
import math

import jax
import jax.numpy as jnp
import numpy as np
from jax import lax
from jax.experimental import pallas as pl
from jax.experimental.pallas import tpu as pltpu
from jax.sharding import PartitionSpec as P

MESH = pl.DeviceIdType.MESH
f32, bf16 = jnp.float32, jnp.bfloat16


PLACES = (0, 1, 4, 5, 2, 3, 6, 7)
EARLY = 4


def signed(count):
    j = np.arange(count)
    return np.where(j < count // 2, j, j - count)


def high_low(table):
    high = table.astype(np.float32).astype(bf16)
    low = (table - high.astype(np.float64)).astype(np.float32).astype(bf16)
    return high, low


def tables(n, keep, devices):
    k = signed(keep)
    phase = 2.0 * math.pi / n * np.mod(k[:, None] * np.arange(n)[None, :], n)
    cos, sin = np.cos(phase) / math.sqrt(n), np.sin(phase) / math.sqrt(n)
    half = keep // 2
    tx = []
    for b in range(2):
        rows = slice(b * half, (b + 1) * half)
        high, low = high_low(np.concatenate([cos[rows].T, -sin[rows].T], axis=1))
        tx.append(np.concatenate([high, low, high], axis=0))
    ty = []
    for p in range(2):
        high, low = high_low(np.concatenate([cos[p::2, : n // 2], sin[p::2, : n // 2]], axis=0))
        ty.append(np.concatenate([high, low, high], axis=1))
    order = np.arange(n).reshape(devices, n // devices).T.reshape(-1)
    high, low = high_low(np.concatenate([cos[:, order], sin[:, order]], axis=0))
    tz = np.concatenate([high, low, high], axis=1)
    return np.stack(tx), np.stack(ty), tz


def split(x):
    high = x.astype(bf16)
    return high, (x - high.astype(f32)).astype(bf16)


def kernel(
    dims, v_hbm, w_hbm, m_hbm, tx_hbm, ty_hbm, tz_hbm, out, viscous,
    v, w, modes, tx, ty, tz, own, away, arrived, outbox, inbox, spec,
    in_sem, m_sem, t_sem, xs_sem, xr_sem, self_sem, s_sem, r_sem, plane_sem, all_sem,
):
    ny, nz, nx, planes, keep, n = dims
    half = keep // 2
    group = ny * nz * nx
    quad = 4 * planes
    me = lax.axis_index("section") * (group // 2) + lax.axis_index("pen")
    slab = lax.axis_index("slab")
    mx, mz, my = me & (nx - 1), (me // nx) & (nz - 1), me // (nx * nz)

    def device(t, s):
        return {"section": t // (group // 2), "pen": t & (group // 2 - 1), "slab": s}

    far_first = [nz // 2 + ((j + 1) // 2) * (2 * (j % 2) - 1) for j in range(nz)]

    def far(j, count):
        return count // 2 + ((j + 1) // 2) * (2 * (j & 1) - 1)

    def each_peer(body, first=0, last=nx * ny, near=False):
        turn = far_first[::-1] if near else far_first

        def step(i, carry):
            if near:
                i = nx * ny - 1 - i
            ty = (my + far(i // nx, ny)) & (ny - 1)
            tx = (mx + far(i & (nx - 1), nx)) & (nx - 1)
            for dz in turn:
                body(ty * (nx * nz) + ((mz + dz) & (nz - 1)) * nx + tx)
            return carry

        def own_line():
            for dz in turn:
                if dz % nz:
                    body(me - mz * nx + ((mz + dz) & (nz - 1)) * nx)

        if near:
            if last == nx * ny:
                own_line()
            lax.fori_loop(max(nx * ny - last, 1), nx * ny - first, step, 0)
        else:
            lax.fori_loop(first, min(last, nx * ny - 1), step, 0)
            if last == nx * ny:
                own_line()

    def each_peer_by_place(body):
        def step(i, carry, corner):
            ty = (my + far(i // nx, ny)) & (ny - 1)
            tx = (mx + far(i & (nx - 1), nx)) & (nx - 1)
            for z in range(EARLY) if corner else PLACES:
                t = (ty * nz + z) * nx + tx
                if corner or z < EARLY:
                    wanted = ((tx == 0) | (ty == 0)) == corner

                    @pl.when(wanted & (me != t))
                    def _(t=t):
                        body(t)
                else:

                    @pl.when(me != t)
                    def _(t=t):
                        body(t)

            return carry

        for corner in (True, False):
            lax.fori_loop(0, nx * ny, functools.partial(step, corner=corner), 0)

    x_table = pltpu.make_async_copy(tx_hbm, tx, t_sem.at[0])
    y_table = pltpu.make_async_copy(ty_hbm, ty, t_sem.at[1])
    z_table = pltpu.make_async_copy(tz_hbm, tz, t_sem.at[2])
    mode_load = pltpu.make_async_copy(m_hbm, modes, m_sem)
    fields = [
        [
            pltpu.make_async_copy(src.at[c, z], dst.at[c, z], in_sem.at[4 * z + i])
            for i, (src, dst, c) in enumerate(
                ((v_hbm, v, 1), (w_hbm, w, 2), (v_hbm, v, 2), (w_hbm, w, 1))
            )
        ]
        for z in range(planes)
    ] + [
        [
            pltpu.make_async_copy(src.at[0], dst.at[0], in_sem.at[4 * planes + i])
            for i, (src, dst) in enumerate(((v_hbm, v), (w_hbm, w)))
        ]
    ]

    def start(*copies):
        for copy in copies:
            copy.start()

    start(*fields[0], x_table)

    barrier = pltpu.get_barrier_semaphore()

    def greet(t, semaphore, s=slab):
        pl.semaphore_signal(semaphore, inc=1, device_id=device(t, s), device_id_type=MESH)

    def across_z():
        return [my * (nx * nz) + ((mz + d) & (nz - 1)) * nx + mx for d in far_first if d % nz]

    def across_x():
        return [me - mx + ((mx + d) & (nx - 1)) for d in (2, 1, 3)]

    def across_y():
        return [((my + d) & (ny - 1)) * (nx * nz) + mz * nx + mx for d in (2, 1, 3)]

    with jax.named_scope("greet"):
        lines = across_z() + across_x() + across_y()
        for t in lines:
            greet(t, barrier)
        greet(me, barrier, 1 - slab)
    start(*fields[1])

    def swap(p):
        return pltpu.make_async_remote_copy(
            src_ref=away.at[p],
            dst_ref=arrived.at[p],
            send_sem=xs_sem.at[p],
            recv_sem=xr_sem.at[p],
            device_id=device(me, 1 - slab),
            device_id_type=MESH,
        )

    def x_plane(c, z):
        a, b = (c + 1) % 3, (c + 2) % 3
        p = v[a, z] * w[b, z] - v[b, z] * w[a, z]
        high, low = split(p)
        lhs = jnp.concatenate([high, high, low], axis=1)
        away[c * planes + z] = jnp.dot(lhs, tx[1 - slab], preferred_element_type=f32)
        own[c * planes + z] = jnp.dot(lhs, tx[slab], preferred_element_type=f32)

    sign = (1 - 2 * slab).astype(f32)

    widths = (quad, quad + 2 * planes, 2 * planes)
    bases = (0, group * widths[0], group * (widths[0] + widths[1]))

    def row_of(c, z, q, part):
        if c < 2:
            return bases[c], widths[c], z * 4 + q * 2 + part
        return bases[1 + q], widths[1 + q], (1 - q) * quad + z * 2 + part

    def rows_of(c, z, q, part):
        base, width, row = row_of(c, z, q, part)
        return pl.ds(base + row, group, stride=width)

    def y_plane(c, z):
        p = c * planes + z
        swap(p).wait_recv()
        mine, other = own[p], arrived[p]
        for q, folded in enumerate((mine + other, sign * (mine - other))):
            high, low = split(folded)
            both = jnp.dot(
                ty[q],
                jnp.concatenate([high, high, low], axis=0),
                preferred_element_type=f32,
            )
            outbox[rows_of(c, z, q, 0), :] = (
                both[:half, :half] + both[half:, half:]
            )
            outbox[rows_of(c, z, q, 1), :] = (
                both[:half, half:] - both[half:, :half]
            )

    def message(part, t, row, rows):
        return pl.ds(bases[part] + t * widths[part] + row, rows)

    def send(part, row=0, rows=None, by_place=False, **which):
        rows = rows or widths[part]

        def one(t):
            pltpu.make_async_remote_copy(
                src_ref=outbox.at[message(part, t, row, rows)],
                dst_ref=inbox.at[message(part, me, row, rows)],
                send_sem=s_sem.at[part],
                recv_sem=r_sem.at[part],
                device_id=device(t, slab),
                device_id_type=MESH,
            ).start()

        with jax.named_scope("send"):
            (each_peer_by_place if by_place else each_peer)(one, **which)

    def keep_own(part):
        mine = message(part, me, 0, widths[part])
        return pltpu.make_async_copy(outbox.at[mine], inbox.at[mine], self_sem.at[part])

    def all_of(part, sem):
        some = pl.ds(bases[part], (group - 1) * widths[part])
        return pltpu.make_async_copy(outbox.at[some], inbox.at[some], sem.at[part])

    def looped(body, c):
        def step(z, carry):
            body(c, z)
            return carry

        lax.fori_loop(0, planes, step, 0)

    with jax.named_scope("x0"):
        for z in range(planes):
            for copy in fields[z]:
                copy.wait()
            if z == 0:
                x_table.wait()
                start(*fields[2], y_table, *fields[3])
            x_plane(0, z)
            if z == 1:
                with jax.named_scope("lines"):
                    pl.semaphore_wait(barrier, len(lines) + 1)
                for t in across_x():
                    greet(t, plane_sem)
                swap(0).start()
            if z > 0:
                swap(z).start()
    start(z_table, mode_load)

    plane = nx * (ny - 1)
    y_table.wait()
    with jax.named_scope("plane"):
        pl.semaphore_wait(plane_sem, nx - 1)
    for t in across_y():
        greet(t, all_sem)
    for z in range(planes):
        with jax.named_scope("y0"):
            y_plane(0, z)
        send(0, z * 4, 4, first=plane, near=True)
    with jax.named_scope("all"):
        pl.semaphore_wait(all_sem, ny - 1)
    send(0, last=plane, near=True)
    keep_own(0).start()
    for copy in fields[planes]:
        copy.wait()
    for z in range(planes):
        x_plane(1, z)
        swap(planes + z).start()
    with jax.named_scope("y1"):
        looped(y_plane, 1)
    with jax.named_scope("x2"):
        looped(x_plane, 2)
    for z in range(planes):
        swap(2 * planes + z).start()
    with jax.named_scope("y2"):
        looped(y_plane, 2)
    send(1)
    keep_own(1).start()
    send(2, by_place=True)
    keep_own(2).start()

    limit = -half
    visc = 0.5 / half**2
    to_wave = lambda j: jnp.where(j < half, j, j - keep)
    kz = to_wave(lax.broadcasted_iota(jnp.int32, (keep, half), 0))
    kx = to_wave(slab * half + lax.broadcasted_iota(jnp.int32, (keep, half), 1))

    def waves_of(q):
        ky = jnp.full((keep, half), to_wave(2 * me + q), jnp.int32)
        kept = ((kx != limit) & (ky != limit) & (kz != limit)).astype(f32)
        waves = (kx.astype(f32), ky.astype(f32), kz.astype(f32))
        ksq = waves[0] * waves[0] + waves[1] * waves[1] + waves[2] * waves[2]
        return waves, ksq, kept

    mode_load.wait()
    with jax.named_scope("viscous"):
        for q in range(2):
            _, ksq, _ = waves_of(q)
            for part in range(2):
                rows = pl.ds(2 * q + part, keep, stride=4)
                for c in range(3):
                    viscous[c, rows, :] = visc * ksq * modes[c, rows, :]
    z_table.wait()

    def z_rows(c, q):
        pieces = [
            jnp.concatenate([inbox[rows_of(c, r, q, part), :] for r in range(planes)], axis=0)
            for part in range(2)
        ]
        high, low = split(jnp.concatenate(pieces, axis=1))
        parts = jnp.concatenate([high, high, low], axis=0)
        cos = jnp.dot(tz[:keep], parts, preferred_element_type=f32)
        sin = jnp.dot(tz[keep:], parts, preferred_element_type=f32)
        spec[c, 2 * q] = cos[:, :half] + sin[:, half:]
        spec[c, 2 * q + 1] = cos[:, half:] - sin[:, :half]

    def project(q):
        waves, ksq, kept = waves_of(q)
        scale = 1.0 / jnp.maximum(ksq, 1.0)
        for part in range(2):
            row = 2 * q + part
            s = [spec[c, row] for c in range(3)]
            inner = (waves[0] * s[0] + waves[1] * s[1] + waves[2] * s[2]) * scale
            for c in range(3):
                out[c, pl.ds(row, keep, stride=4), :] = (s[c] - waves[c] * inner) * kept

    for part, ready in enumerate((((0, 0), (0, 1)), ((1, 0), (1, 1), (2, 0)), ((2, 1),))):
        with jax.named_scope("recv"):
            keep_own(part).wait()
            all_of(part, r_sem).wait()
        with jax.named_scope("z"):
            for c, q in ready:
                z_rows(c, q)
        if part:
            with jax.named_scope("project"):
                project(part - 1)

    with jax.named_scope("drain"):
        for p in range(3 * planes):
            swap(p).wait_send()
        for part in range(3):
            all_of(part, s_sem).wait()


def per_device(sizes, velocity, vorticity, velocity_modes):
    ny, nz, nx = sizes
    _, planes, rows, n = velocity.shape
    keep, half = velocity_modes.shape[1], velocity_modes.shape[4]
    group = ny * nz * nx
    tx, ty, tz = tables(n, keep, group)
    quad = 4 * planes
    dma = pltpu.SemaphoreType.DMA
    whole = jax.ShapeDtypeStruct((3, 4 * keep, half), f32)
    operands = (velocity, vorticity, velocity_modes.reshape(whole.shape), tx, ty, tz)
    projected, viscous = pl.pallas_call(
        functools.partial(kernel, (ny, nz, nx, planes, keep, n)),
        out_shape=(whole, whole),
        in_specs=[pl.BlockSpec(memory_space=pltpu.HBM)] * 6,
        out_specs=(pl.BlockSpec(memory_space=pltpu.VMEM),) * 2,
        scratch_shapes=[
            pltpu.VMEM((3, planes, rows, n), f32),
            pltpu.VMEM((3, planes, rows, n), f32),
            pltpu.VMEM(whole.shape, f32),
            pltpu.VMEM(tx.shape, bf16),
            pltpu.VMEM(ty.shape, bf16),
            pltpu.VMEM(tz.shape, bf16),
            pltpu.VMEM((3 * planes, rows, keep), f32),
            pltpu.VMEM((3 * planes, rows, keep), f32),
            pltpu.VMEM((3 * planes, rows, keep), f32),
            pltpu.VMEM((3 * group * quad, half), f32),
            pltpu.VMEM((3 * group * quad, half), f32),
            pltpu.VMEM((3, 4, keep, half), f32),
            dma((4 * planes + 2,)),
            dma,
            dma((3,)),
            dma((3 * planes,)),
            dma((3 * planes,)),
            dma((3,)),
            dma((3,)),
            dma((3,)),
            pltpu.SemaphoreType.REGULAR,
            pltpu.SemaphoreType.REGULAR,
        ],
        compiler_params=pltpu.CompilerParams(
            collective_id=0, has_side_effects=True, vmem_limit_bytes=30 << 20
        ),
    )(*(pltpu.with_memory_space_constraint(x, pltpu.HBM) for x in operands))
    return (projected - viscous).reshape(velocity_modes.shape)


def solution(mesh):
    sizes = (4, 8, 4)
    return jax.shard_map(
        functools.partial(per_device, sizes),
        mesh=mesh,
        in_specs=(
            P(None, ("section", "pen"), "slab", None),
            P(None, ("section", "pen"), "slab", None),
            P(None, None, ("section", "pen"), None, "slab"),
        ),
        out_specs=P(None, None, ("section", "pen"), None, "slab"),
        check_vma=False,
    )
```

```python
import functools
import math

import jax
import jax.numpy as jnp
import numpy as np
from jax import lax
from jax.experimental import pallas as pl
from jax.experimental.pallas import tpu as pltpu
from jax.sharding import PartitionSpec as P

MESH = pl.DeviceIdType.MESH
f32, bf16 = jnp.float32, jnp.bfloat16


PLACES = (0, 1, 4, 5, 2, 3, 6, 7)
EARLY = 4


def signed(count):
    j = np.arange(count)
    return np.where(j < count // 2, j, j - count)


def high_low(table):
    high = table.astype(np.float32).astype(bf16)
    low = (table - high.astype(np.float64)).astype(np.float32).astype(bf16)
    return high, low


def tables(n, keep, devices):
    k = signed(keep)
    phase = 2.0 * math.pi / n * np.mod(k[:, None] * np.arange(n)[None, :], n)
    cos, sin = np.cos(phase) / math.sqrt(n), np.sin(phase) / math.sqrt(n)
    half = keep // 2
    tx = []
    for b in range(2):
        rows = slice(b * half, (b + 1) * half)
        high, low = high_low(np.concatenate([cos[rows].T, -sin[rows].T], axis=1))
        tx.append(np.concatenate([high, low, high], axis=0))
    ty = []
    for p in range(2):
        high, low = high_low(np.concatenate([cos[p::2, : n // 2], sin[p::2, : n // 2]], axis=0))
        ty.append(np.concatenate([high, low, high], axis=1))
    order = np.arange(n).reshape(devices, n // devices).T.reshape(-1)
    high, low = high_low(np.concatenate([cos[:, order], sin[:, order]], axis=0))
    tz = np.concatenate([high, low, high], axis=1)
    return np.stack(tx), np.stack(ty), tz


def split(x):
    high = x.astype(bf16)
    return high, (x - high.astype(f32)).astype(bf16)


def kernel(
    dims, v_hbm, w_hbm, m_hbm, tx_hbm, ty_hbm, tz_hbm, out,
    v, w, modes, tx, ty, tz, own, away, arrived, outbox, inbox, spec,
    in_sem, m_sem, t_sem, xs_sem, xr_sem, self_sem, s_sem, r_sem, plane_sem, all_sem,
):
    ny, nz, nx, planes, keep, n = dims
    half = keep // 2
    group = ny * nz * nx
    quad = 4 * planes
    me = lax.axis_index("section") * (group // 2) + lax.axis_index("pen")
    slab = lax.axis_index("slab")
    mx, mz, my = me & (nx - 1), (me // nx) & (nz - 1), me // (nx * nz)

    def device(t, s):
        return {"section": t // (group // 2), "pen": t & (group // 2 - 1), "slab": s}

    far_first = [nz // 2 + ((j + 1) // 2) * (2 * (j % 2) - 1) for j in range(nz)]

    def far(j, count):
        return count // 2 + ((j + 1) // 2) * (2 * (j & 1) - 1)

    def each_peer(body, first=0, last=nx * ny, near=False):
        turn = far_first[::-1] if near else far_first

        def step(i, carry):
            if near:
                i = nx * ny - 1 - i
            ty = (my + far(i // nx, ny)) & (ny - 1)
            tx = (mx + far(i & (nx - 1), nx)) & (nx - 1)
            for dz in turn:
                body(ty * (nx * nz) + ((mz + dz) & (nz - 1)) * nx + tx)
            return carry

        def own_line():
            for dz in turn:
                if dz % nz:
                    body(me - mz * nx + ((mz + dz) & (nz - 1)) * nx)

        if near:
            if last == nx * ny:
                own_line()
            lax.fori_loop(max(nx * ny - last, 1), nx * ny - first, step, 0)
        else:
            lax.fori_loop(first, min(last, nx * ny - 1), step, 0)
            if last == nx * ny:
                own_line()

    def each_peer_by_place(body):
        def step(i, carry, corner):
            ty = (my + far(i // nx, ny)) & (ny - 1)
            tx = (mx + far(i & (nx - 1), nx)) & (nx - 1)
            for z in range(EARLY) if corner else PLACES:
                t = (ty * nz + z) * nx + tx
                if corner or z < EARLY:
                    wanted = ((tx == 0) | (ty == 0)) == corner

                    @pl.when(wanted & (me != t))
                    def _(t=t):
                        body(t)
                else:

                    @pl.when(me != t)
                    def _(t=t):
                        body(t)

            return carry

        for corner in (True, False):
            lax.fori_loop(0, nx * ny, functools.partial(step, corner=corner), 0)

    x_table = pltpu.make_async_copy(tx_hbm, tx, t_sem.at[0])
    y_table = pltpu.make_async_copy(ty_hbm, ty, t_sem.at[1])
    z_table = pltpu.make_async_copy(tz_hbm, tz, t_sem.at[2])
    mode_load = pltpu.make_async_copy(m_hbm, modes, m_sem)
    fields = [
        [
            pltpu.make_async_copy(src.at[c, z], dst.at[c, z], in_sem.at[4 * z + i])
            for i, (src, dst, c) in enumerate(
                ((v_hbm, v, 1), (w_hbm, w, 2), (v_hbm, v, 2), (w_hbm, w, 1))
            )
        ]
        for z in range(planes)
    ] + [
        [
            pltpu.make_async_copy(src.at[0], dst.at[0], in_sem.at[4 * planes + i])
            for i, (src, dst) in enumerate(((v_hbm, v), (w_hbm, w)))
        ]
    ]

    def start(*copies):
        for copy in copies:
            copy.start()

    start(*fields[0], x_table)

    barrier = pltpu.get_barrier_semaphore()

    def greet(t, semaphore, s=slab):
        pl.semaphore_signal(semaphore, inc=1, device_id=device(t, s), device_id_type=MESH)

    def across_z():
        return [my * (nx * nz) + ((mz + d) & (nz - 1)) * nx + mx for d in far_first if d % nz]

    def across_x():
        return [me - mx + ((mx + d) & (nx - 1)) for d in (2, 1, 3)]

    def across_y():
        return [((my + d) & (ny - 1)) * (nx * nz) + mz * nx + mx for d in (2, 1, 3)]

    with jax.named_scope("greet"):
        lines = across_z() + across_x() + across_y()
        for t in lines:
            greet(t, barrier)
        greet(me, barrier, 1 - slab)
    start(*fields[1])

    def swap(p):
        return pltpu.make_async_remote_copy(
            src_ref=away.at[p],
            dst_ref=arrived.at[p],
            send_sem=xs_sem.at[p],
            recv_sem=xr_sem.at[p],
            device_id=device(me, 1 - slab),
            device_id_type=MESH,
        )

    def x_plane(c, z):
        a, b = (c + 1) % 3, (c + 2) % 3
        p = v[a, z] * w[b, z] - v[b, z] * w[a, z]
        high, low = split(p)
        lhs = jnp.concatenate([high, high, low], axis=1)
        away[c * planes + z] = jnp.dot(lhs, tx[1 - slab], preferred_element_type=f32)
        own[c * planes + z] = jnp.dot(lhs, tx[slab], preferred_element_type=f32)

    sign = (1 - 2 * slab).astype(f32)

    widths = (quad, quad + 2 * planes, 2 * planes)
    bases = (0, group * widths[0], group * (widths[0] + widths[1]))

    def row_of(c, z, q, part):
        if c < 2:
            return bases[c], widths[c], z * 4 + q * 2 + part
        return bases[1 + q], widths[1 + q], (1 - q) * quad + z * 2 + part

    def rows_of(c, z, q, part):
        base, width, row = row_of(c, z, q, part)
        return pl.ds(base + row, group, stride=width)

    def y_plane(c, z):
        p = c * planes + z
        swap(p).wait_recv()
        mine, other = own[p], arrived[p]
        for q, folded in enumerate((mine + other, sign * (mine - other))):
            high, low = split(folded)
            both = jnp.dot(
                ty[q],
                jnp.concatenate([high, high, low], axis=0),
                preferred_element_type=f32,
            )
            outbox[rows_of(c, z, q, 0), :] = (
                both[:half, :half] + both[half:, half:]
            )
            outbox[rows_of(c, z, q, 1), :] = (
                both[:half, half:] - both[half:, :half]
            )

    def message(part, t, row, rows):
        return pl.ds(bases[part] + t * widths[part] + row, rows)

    def send(part, row=0, rows=None, by_place=False, **which):
        rows = rows or widths[part]

        def one(t):
            pltpu.make_async_remote_copy(
                src_ref=outbox.at[message(part, t, row, rows)],
                dst_ref=inbox.at[message(part, me, row, rows)],
                send_sem=s_sem.at[part],
                recv_sem=r_sem.at[part],
                device_id=device(t, slab),
                device_id_type=MESH,
            ).start()

        with jax.named_scope("send"):
            (each_peer_by_place if by_place else each_peer)(one, **which)

    def keep_own(part):
        mine = message(part, me, 0, widths[part])
        return pltpu.make_async_copy(outbox.at[mine], inbox.at[mine], self_sem.at[part])

    def all_of(part, sem):
        some = pl.ds(bases[part], (group - 1) * widths[part])
        return pltpu.make_async_copy(outbox.at[some], inbox.at[some], sem.at[part])

    def looped(body, c):
        def step(z, carry):
            body(c, z)
            return carry

        lax.fori_loop(0, planes, step, 0)

    with jax.named_scope("x0"):
        for z in range(planes):
            for copy in fields[z]:
                copy.wait()
            if z == 0:
                x_table.wait()
                start(*fields[2], y_table, *fields[3])
            x_plane(0, z)
            if z == 1:
                with jax.named_scope("lines"):
                    pl.semaphore_wait(barrier, len(lines) + 1)
                for t in across_x():
                    greet(t, plane_sem)
                swap(0).start()
            if z > 0:
                swap(z).start()
    start(z_table, mode_load)

    plane = nx * (ny - 1)
    y_table.wait()
    with jax.named_scope("plane"):
        pl.semaphore_wait(plane_sem, nx - 1)
    for t in across_y():
        greet(t, all_sem)
    for z in range(planes):
        with jax.named_scope("y0"):
            y_plane(0, z)
        send(0, z * 4, 4, first=plane, near=True)
    with jax.named_scope("all"):
        pl.semaphore_wait(all_sem, ny - 1)
    send(0, last=plane, near=True)
    keep_own(0).start()
    for copy in fields[planes]:
        copy.wait()
    for z in range(planes):
        x_plane(1, z)
        swap(planes + z).start()
    with jax.named_scope("y1"):
        looped(y_plane, 1)
    with jax.named_scope("x2"):
        looped(x_plane, 2)
    for z in range(planes):
        swap(2 * planes + z).start()
    with jax.named_scope("y2"):
        looped(y_plane, 2)
    send(1, near=True)
    keep_own(1).start()
    send(2, by_place=True)
    keep_own(2).start()

    limit = -half
    visc = 0.5 / half**2
    to_wave = lambda j: jnp.where(j < half, j, j - keep)
    kz = to_wave(lax.broadcasted_iota(jnp.int32, (keep, half), 0))
    kx = to_wave(slab * half + lax.broadcasted_iota(jnp.int32, (keep, half), 1))

    def waves_of(q):
        ky = jnp.full((keep, half), to_wave(2 * me + q), jnp.int32)
        kept = ((kx != limit) & (ky != limit) & (kz != limit)).astype(f32)
        waves = (kx.astype(f32), ky.astype(f32), kz.astype(f32))
        ksq = waves[0] * waves[0] + waves[1] * waves[1] + waves[2] * waves[2]
        return waves, ksq, kept

    mode_load.wait()
    z_table.wait()

    def z_rows(c, q):
        pieces = [
            jnp.concatenate([inbox[rows_of(c, r, q, part), :] for r in range(planes)], axis=0)
            for part in range(2)
        ]
        high, low = split(jnp.concatenate(pieces, axis=1))
        parts = jnp.concatenate([high, high, low], axis=0)
        cos = jnp.dot(tz[:keep], parts, preferred_element_type=f32)
        sin = jnp.dot(tz[keep:], parts, preferred_element_type=f32)
        spec[c, 2 * q] = cos[:, :half] + sin[:, half:]
        spec[c, 2 * q + 1] = cos[:, half:] - sin[:, :half]

    def project(q):
        waves, ksq, kept = waves_of(q)
        scale = 1.0 / jnp.maximum(ksq, 1.0)
        for part in range(2):
            row = 2 * q + part
            s = [spec[c, row] for c in range(3)]
            inner = (waves[0] * s[0] + waves[1] * s[1] + waves[2] * s[2]) * scale
            for c in range(3):
                rows = pl.ds(row, keep, stride=4)
                out[c, rows, :] = (s[c] - waves[c] * inner) * kept - visc * ksq * modes[c, rows, :]

    for part, ready in enumerate((((0, 0), (0, 1)), ((1, 0), (1, 1), (2, 0)), ((2, 1),))):
        with jax.named_scope("recv"):
            keep_own(part).wait()
            all_of(part, r_sem).wait()
        with jax.named_scope("z"):
            for c, q in ready:
                z_rows(c, q)
        if part:
            with jax.named_scope("project"):
                project(part - 1)

    with jax.named_scope("drain"):
        for p in range(3 * planes):
            swap(p).wait_send()
        for part in range(3):
            all_of(part, s_sem).wait()


def leave(held, out, sem):
    pieces = [(c, pl.ds(h * 512, 512)) for c in range(3) for h in range(2)]
    copies = [
        pltpu.make_async_copy(held.at[c, rows], out.at[c, rows], sem.at[i])
        for i, (c, rows) in enumerate(pieces)
    ]
    for copy in copies:
        copy.start()
    for copy in copies:
        copy.wait()


def per_device(sizes, velocity, vorticity, velocity_modes):
    ny, nz, nx = sizes
    _, planes, rows, n = velocity.shape
    keep, half = velocity_modes.shape[1], velocity_modes.shape[4]
    group = ny * nz * nx
    tx, ty, tz = tables(n, keep, group)
    quad = 4 * planes
    dma = pltpu.SemaphoreType.DMA
    whole = jax.ShapeDtypeStruct((3, 4 * keep, half), f32)
    operands = (velocity, vorticity, velocity_modes.reshape(whole.shape), tx, ty, tz)
    held = pl.pallas_call(
        functools.partial(kernel, (ny, nz, nx, planes, keep, n)),
        out_shape=whole,
        in_specs=[pl.BlockSpec(memory_space=pltpu.HBM)] * 6,
        out_specs=pl.BlockSpec(memory_space=pltpu.VMEM),
        scratch_shapes=[
            pltpu.VMEM((3, planes, rows, n), f32),
            pltpu.VMEM((3, planes, rows, n), f32),
            pltpu.VMEM(whole.shape, f32),
            pltpu.VMEM(tx.shape, bf16),
            pltpu.VMEM(ty.shape, bf16),
            pltpu.VMEM(tz.shape, bf16),
            pltpu.VMEM((3 * planes, rows, keep), f32),
            pltpu.VMEM((3 * planes, rows, keep), f32),
            pltpu.VMEM((3 * planes, rows, keep), f32),
            pltpu.VMEM((3 * group * quad, half), f32),
            pltpu.VMEM((3 * group * quad, half), f32),
            pltpu.VMEM((3, 4, keep, half), f32),
            dma((4 * planes + 2,)),
            dma,
            dma((3,)),
            dma((3 * planes,)),
            dma((3 * planes,)),
            dma((3,)),
            dma((3,)),
            dma((3,)),
            pltpu.SemaphoreType.REGULAR,
            pltpu.SemaphoreType.REGULAR,
        ],
        compiler_params=pltpu.CompilerParams(
            collective_id=0, has_side_effects=True, vmem_limit_bytes=30 << 20
        ),
    )(*(pltpu.with_memory_space_constraint(x, pltpu.HBM) for x in operands))
    out = pl.pallas_call(
        leave,
        out_shape=whole,
        in_specs=[pl.BlockSpec(memory_space=pltpu.VMEM)],
        out_specs=pl.BlockSpec(memory_space=pltpu.HBM),
        scratch_shapes=[dma((6,))],
        compiler_params=pltpu.CompilerParams(vmem_limit_bytes=4 << 20),
    )(held)
    return out.reshape(velocity_modes.shape)


def solution(mesh):
    sizes = (4, 8, 4)
    return jax.shard_map(
        functools.partial(per_device, sizes),
        mesh=mesh,
        in_specs=(
            P(None, ("section", "pen"), "slab", None),
            P(None, ("section", "pen"), "slab", None),
            P(None, None, ("section", "pen"), None, "slab"),
        ),
        out_specs=P(None, None, ("section", "pen"), None, "slab"),
        check_vma=False,
    )
```

```python
import functools
import math

import jax
import jax.numpy as jnp
import numpy as np
from jax import lax
from jax.experimental import pallas as pl
from jax.experimental.pallas import tpu as pltpu
from jax.sharding import PartitionSpec as P

MESH = pl.DeviceIdType.MESH
f32, bf16 = jnp.float32, jnp.bfloat16


PLACES = (0, 1, 4, 5, 2, 3, 6, 7)
EARLY = 4


def signed(count):
    j = np.arange(count)
    return np.where(j < count // 2, j, j - count)


def high_low(table):
    high = table.astype(np.float32).astype(bf16)
    low = (table - high.astype(np.float64)).astype(np.float32).astype(bf16)
    return high, low


def tables(n, keep, devices):
    k = signed(keep)
    phase = 2.0 * math.pi / n * np.mod(k[:, None] * np.arange(n)[None, :], n)
    cos, sin = np.cos(phase) / math.sqrt(n), np.sin(phase) / math.sqrt(n)
    half = keep // 2
    tx = []
    for b in range(2):
        rows = slice(b * half, (b + 1) * half)
        high, low = high_low(np.concatenate([cos[rows].T, -sin[rows].T], axis=1))
        tx.append(np.concatenate([high, low, high], axis=0))
    ty = []
    for p in range(2):
        high, low = high_low(np.concatenate([cos[p::2, : n // 2], sin[p::2, : n // 2]], axis=0))
        ty.append(np.concatenate([high, low, high], axis=1))
    order = np.arange(n).reshape(devices, n // devices).T.reshape(-1)
    high, low = high_low(np.concatenate([cos[:, order], sin[:, order]], axis=0))
    tz = np.concatenate([high, low, high], axis=1)
    return np.stack(tx), np.stack(ty), tz


def split(x):
    high = x.astype(bf16)
    return high, (x - high.astype(f32)).astype(bf16)


def kernel(
    dims, v_hbm, w_hbm, m_hbm, tx_hbm, ty_hbm, tz_hbm, out, viscous,
    v, w, modes, tx, ty, tz, own, away, arrived, outbox, inbox, spec,
    in_sem, m_sem, t_sem, xs_sem, xr_sem, self_sem, s_sem, r_sem, plane_sem, all_sem,
):
    ny, nz, nx, planes, keep, n = dims
    half = keep // 2
    group = ny * nz * nx
    quad = 4 * planes
    me = lax.axis_index("section") * (group // 2) + lax.axis_index("pen")
    slab = lax.axis_index("slab")
    mx, mz, my = me & (nx - 1), (me // nx) & (nz - 1), me // (nx * nz)

    def device(t, s):
        return {"section": t // (group // 2), "pen": t & (group // 2 - 1), "slab": s}

    far_first = [nz // 2 + ((j + 1) // 2) * (2 * (j % 2) - 1) for j in range(nz)]

    def far(j, count):
        return count // 2 + ((j + 1) // 2) * (2 * (j & 1) - 1)

    def each_peer(body, first=0, last=nx * ny, near=False):
        turn = far_first[::-1] if near else far_first

        def step(i, carry):
            if near:
                i = nx * ny - 1 - i
            ty = (my + far(i // nx, ny)) & (ny - 1)
            tx = (mx + far(i & (nx - 1), nx)) & (nx - 1)
            for dz in turn:
                body(ty * (nx * nz) + ((mz + dz) & (nz - 1)) * nx + tx)
            return carry

        def own_line():
            for dz in turn:
                if dz % nz:
                    body(me - mz * nx + ((mz + dz) & (nz - 1)) * nx)

        if near:
            if last == nx * ny:
                own_line()
            lax.fori_loop(max(nx * ny - last, 1), nx * ny - first, step, 0)
        else:
            lax.fori_loop(first, min(last, nx * ny - 1), step, 0)
            if last == nx * ny:
                own_line()

    def each_peer_by_place(body):
        def step(i, carry, corner):
            ty = (my + far(i // nx, ny)) & (ny - 1)
            tx = (mx + far(i & (nx - 1), nx)) & (nx - 1)
            for z in range(EARLY) if corner else PLACES:
                t = (ty * nz + z) * nx + tx
                if corner or z < EARLY:
                    wanted = ((tx == 0) | (ty == 0)) == corner

                    @pl.when(wanted & (me != t))
                    def _(t=t):
                        body(t)
                else:

                    @pl.when(me != t)
                    def _(t=t):
                        body(t)

            return carry

        for corner in (True, False):
            lax.fori_loop(0, nx * ny, functools.partial(step, corner=corner), 0)

    x_table = pltpu.make_async_copy(tx_hbm, tx, t_sem.at[0])
    y_table = pltpu.make_async_copy(ty_hbm, ty, t_sem.at[1])
    z_table = pltpu.make_async_copy(tz_hbm, tz, t_sem.at[2])
    mode_load = pltpu.make_async_copy(m_hbm, modes, m_sem)
    fields = [
        [
            pltpu.make_async_copy(src.at[c, z], dst.at[c, z], in_sem.at[4 * z + i])
            for i, (src, dst, c) in enumerate(
                ((v_hbm, v, 1), (w_hbm, w, 2), (v_hbm, v, 2), (w_hbm, w, 1))
            )
        ]
        for z in range(planes)
    ] + [
        [
            pltpu.make_async_copy(src.at[0], dst.at[0], in_sem.at[4 * planes + i])
            for i, (src, dst) in enumerate(((v_hbm, v), (w_hbm, w)))
        ]
    ]

    def start(*copies):
        for copy in copies:
            copy.start()

    start(*fields[0], x_table)

    barrier = pltpu.get_barrier_semaphore()

    def greet(t, semaphore, s=slab):
        pl.semaphore_signal(semaphore, inc=1, device_id=device(t, s), device_id_type=MESH)

    def across_z():
        return [my * (nx * nz) + ((mz + d) & (nz - 1)) * nx + mx for d in far_first if d % nz]

    def across_x():
        return [me - mx + ((mx + d) & (nx - 1)) for d in (2, 1, 3)]

    def across_y():
        return [((my + d) & (ny - 1)) * (nx * nz) + mz * nx + mx for d in (2, 1, 3)]

    with jax.named_scope("greet"):
        lines = across_z() + across_x() + across_y()
        for t in lines:
            greet(t, barrier)
        greet(me, barrier, 1 - slab)
    start(*fields[1])

    def swap(p):
        return pltpu.make_async_remote_copy(
            src_ref=away.at[p],
            dst_ref=arrived.at[p],
            send_sem=xs_sem.at[p],
            recv_sem=xr_sem.at[p],
            device_id=device(me, 1 - slab),
            device_id_type=MESH,
        )

    def x_plane(c, z):
        a, b = (c + 1) % 3, (c + 2) % 3
        p = v[a, z] * w[b, z] - v[b, z] * w[a, z]
        high, low = split(p)
        lhs = jnp.concatenate([high, high, low], axis=1)
        away[c * planes + z] = jnp.dot(lhs, tx[1 - slab], preferred_element_type=f32)
        own[c * planes + z] = jnp.dot(lhs, tx[slab], preferred_element_type=f32)

    sign = (1 - 2 * slab).astype(f32)

    widths = (quad, quad + 2 * planes, 2 * planes)
    bases = (0, group * widths[0], group * (widths[0] + widths[1]))

    def row_of(c, z, q, part):
        if c < 2:
            return bases[c], widths[c], z * 4 + q * 2 + part
        return bases[1 + q], widths[1 + q], (1 - q) * quad + z * 2 + part

    def rows_of(c, z, q, part):
        base, width, row = row_of(c, z, q, part)
        return pl.ds(base + row, group, stride=width)

    def y_plane(c, z):
        p = c * planes + z
        swap(p).wait_recv()
        mine, other = own[p], arrived[p]
        for q, folded in enumerate((mine + other, sign * (mine - other))):
            high, low = split(folded)
            both = jnp.dot(
                ty[q],
                jnp.concatenate([high, high, low], axis=0),
                preferred_element_type=f32,
            )
            outbox[rows_of(c, z, q, 0), :] = (
                both[:half, :half] + both[half:, half:]
            )
            outbox[rows_of(c, z, q, 1), :] = (
                both[:half, half:] - both[half:, :half]
            )

    def message(part, t, row, rows):
        return pl.ds(bases[part] + t * widths[part] + row, rows)

    def send(part, row=0, rows=None, by_place=False, **which):
        rows = rows or widths[part]

        def one(t):
            pltpu.make_async_remote_copy(
                src_ref=outbox.at[message(part, t, row, rows)],
                dst_ref=inbox.at[message(part, me, row, rows)],
                send_sem=s_sem.at[part],
                recv_sem=r_sem.at[part],
                device_id=device(t, slab),
                device_id_type=MESH,
            ).start()

        with jax.named_scope("send"):
            (each_peer_by_place if by_place else each_peer)(one, **which)

    def keep_own(part):
        mine = message(part, me, 0, widths[part])
        return pltpu.make_async_copy(outbox.at[mine], inbox.at[mine], self_sem.at[part])

    def all_of(part, sem):
        some = pl.ds(bases[part], (group - 1) * widths[part])
        return pltpu.make_async_copy(outbox.at[some], inbox.at[some], sem.at[part])

    def looped(body, c):
        def step(z, carry):
            body(c, z)
            return carry

        lax.fori_loop(0, planes, step, 0)

    with jax.named_scope("x0"):
        for z in range(planes):
            for copy in fields[z]:
                copy.wait()
            if z == 0:
                x_table.wait()
                start(*fields[2], y_table, *fields[3])
            x_plane(0, z)
            if z == 1:
                with jax.named_scope("lines"):
                    pl.semaphore_wait(barrier, len(lines) + 1)
                for t in across_x():
                    greet(t, plane_sem)
                swap(0).start()
            if z > 0:
                swap(z).start()
    start(z_table, mode_load)

    plane = nx * (ny - 1)
    y_table.wait()
    with jax.named_scope("plane"):
        pl.semaphore_wait(plane_sem, nx - 1)
    for t in across_y():
        greet(t, all_sem)
    for z in range(planes):
        with jax.named_scope("y0"):
            y_plane(0, z)
        send(0, z * 4, 4, first=plane, near=True)
    with jax.named_scope("all"):
        pl.semaphore_wait(all_sem, ny - 1)
    send(0, last=plane)
    keep_own(0).start()
    for copy in fields[planes]:
        copy.wait()
    for z in range(planes):
        x_plane(1, z)
        swap(planes + z).start()
    with jax.named_scope("y1"):
        looped(y_plane, 1)
    with jax.named_scope("x2"):
        looped(x_plane, 2)
    for z in range(planes):
        swap(2 * planes + z).start()
    with jax.named_scope("y2"):
        looped(y_plane, 2)
    send(1, near=True)
    keep_own(1).start()
    send(2, by_place=True)
    keep_own(2).start()

    limit = -half
    visc = 0.5 / half**2
    to_wave = lambda j: jnp.where(j < half, j, j - keep)
    kz = to_wave(lax.broadcasted_iota(jnp.int32, (keep, half), 0))
    kx = to_wave(slab * half + lax.broadcasted_iota(jnp.int32, (keep, half), 1))

    def waves_of(q):
        ky = jnp.full((keep, half), to_wave(2 * me + q), jnp.int32)
        kept = ((kx != limit) & (ky != limit) & (kz != limit)).astype(f32)
        waves = (kx.astype(f32), ky.astype(f32), kz.astype(f32))
        ksq = waves[0] * waves[0] + waves[1] * waves[1] + waves[2] * waves[2]
        return waves, ksq, kept

    mode_load.wait()
    with jax.named_scope("viscous"):
        for q in range(2):
            _, ksq, _ = waves_of(q)
            for part in range(2):
                rows = pl.ds(2 * q + part, keep, stride=4)
                for c in range(3):
                    viscous[c, rows, :] = visc * ksq * modes[c, rows, :]
    z_table.wait()

    def z_rows(c, q):
        pieces = [
            jnp.concatenate([inbox[rows_of(c, r, q, part), :] for r in range(planes)], axis=0)
            for part in range(2)
        ]
        high, low = split(jnp.concatenate(pieces, axis=1))
        parts = jnp.concatenate([high, high, low], axis=0)
        cos = jnp.dot(tz[:keep], parts, preferred_element_type=f32)
        sin = jnp.dot(tz[keep:], parts, preferred_element_type=f32)
        spec[c, 2 * q] = cos[:, :half] + sin[:, half:]
        spec[c, 2 * q + 1] = cos[:, half:] - sin[:, :half]

    def project(q):
        waves, ksq, kept = waves_of(q)
        scale = 1.0 / jnp.maximum(ksq, 1.0)
        for part in range(2):
            row = 2 * q + part
            s = [spec[c, row] for c in range(3)]
            inner = (waves[0] * s[0] + waves[1] * s[1] + waves[2] * s[2]) * scale
            for c in range(3):
                out[c, pl.ds(row, keep, stride=4), :] = (s[c] - waves[c] * inner) * kept

    for part, ready in enumerate((((0, 0), (0, 1)), ((1, 0), (1, 1), (2, 0)), ((2, 1),))):
        with jax.named_scope("recv"):
            keep_own(part).wait()
            all_of(part, r_sem).wait()
        with jax.named_scope("z"):
            for c, q in ready:
                z_rows(c, q)
        if part:
            with jax.named_scope("project"):
                project(part - 1)

    with jax.named_scope("drain"):
        for p in range(3 * planes):
            swap(p).wait_send()
        for part in range(3):
            all_of(part, s_sem).wait()


def per_device(sizes, velocity, vorticity, velocity_modes):
    ny, nz, nx = sizes
    _, planes, rows, n = velocity.shape
    keep, half = velocity_modes.shape[1], velocity_modes.shape[4]
    group = ny * nz * nx
    tx, ty, tz = tables(n, keep, group)
    quad = 4 * planes
    dma = pltpu.SemaphoreType.DMA
    whole = jax.ShapeDtypeStruct((3, 4 * keep, half), f32)
    operands = (velocity, vorticity, velocity_modes.reshape(whole.shape), tx, ty, tz)
    projected, viscous = pl.pallas_call(
        functools.partial(kernel, (ny, nz, nx, planes, keep, n)),
        out_shape=(whole, whole),
        in_specs=[pl.BlockSpec(memory_space=pltpu.HBM)] * 6,
        out_specs=(pl.BlockSpec(memory_space=pltpu.VMEM),) * 2,
        scratch_shapes=[
            pltpu.VMEM((3, planes, rows, n), f32),
            pltpu.VMEM((3, planes, rows, n), f32),
            pltpu.VMEM(whole.shape, f32),
            pltpu.VMEM(tx.shape, bf16),
            pltpu.VMEM(ty.shape, bf16),
            pltpu.VMEM(tz.shape, bf16),
            pltpu.VMEM((3 * planes, rows, keep), f32),
            pltpu.VMEM((3 * planes, rows, keep), f32),
            pltpu.VMEM((3 * planes, rows, keep), f32),
            pltpu.VMEM((3 * group * quad, half), f32),
            pltpu.VMEM((3 * group * quad, half), f32),
            pltpu.VMEM((3, 4, keep, half), f32),
            dma((4 * planes + 2,)),
            dma,
            dma((3,)),
            dma((3 * planes,)),
            dma((3 * planes,)),
            dma((3,)),
            dma((3,)),
            dma((3,)),
            pltpu.SemaphoreType.REGULAR,
            pltpu.SemaphoreType.REGULAR,
        ],
        compiler_params=pltpu.CompilerParams(
            collective_id=0, has_side_effects=True, vmem_limit_bytes=30 << 20
        ),
    )(*(pltpu.with_memory_space_constraint(x, pltpu.HBM) for x in operands))
    return (projected - viscous).reshape(velocity_modes.shape)


def solution(mesh):
    sizes = (4, 8, 4)
    return jax.shard_map(
        functools.partial(per_device, sizes),
        mesh=mesh,
        in_specs=(
            P(None, ("section", "pen"), "slab", None),
            P(None, ("section", "pen"), "slab", None),
            P(None, None, ("section", "pen"), None, "slab"),
        ),
        out_specs=P(None, None, ("section", "pen"), None, "slab"),
        check_vma=False,
    )
```
